32 devices in a mesh: gx: 4 (over z), gy: 8 (over y, x, core).
Axes of the slice: x: 2, y: 2, z: 4, core: 2. Of those that a mesh axis runs over, the one named last changes fastest.
Arguments:
- node_coords: float32 [12288, 3, 128], P(('gx', 'gy')), may hold values from -6 to 6
- node_disp: float32 [12288, 3, 128], P(('gx', 'gy')), may hold values from -6 to 6
- qpoints: float32 [8192, 3, 256], P(('gx', 'gy')), may hold values from -6 to 6
- qweights: float32 [8192, 256], P(('gx', 'gy')), may hold values from 0.1 to 2
- qcount: int32 [8192], P(('gx', 'gy')), may hold values from 64 to 256
- sec_block: int32 [8192], P(('gx', 'gy')), may hold values from 0 to 12287, as said below
- pri_block: int32 [8192], P(('gx', 'gy')), may hold values from 0 to 12287, as said below
Outputs:
- gap: float32 [12288, 3, 128], P(('gx', 'gy'))
The draws below stay inside these ranges and needn't reach their ends.
Inputs may be any that keep to these rules, and one draw needn't show every extreme that they name: `sec_block`: patch b is owned by device b // 384. Among the segments of one device, at most 16 have their secondary patch owned by any one device; in every draw some device owns the secondary patches of exactly 16 segments of every device. `pri_block`: as for sec_block, with primary patches: at most 16 segments of one device name patches of any one owner, and some owner gets exactly 16 from every device.
All inputs are finite; a program needn't handle non-finite values.
Results may differ from the reference program's by a relative error of at most 0.000098.
Values sent between devices are 32-bit elements; how exact they have to be, the bound alone decides.
A program may use at most 64 MiB of HBM per device.

```python
import math
import jax
import jax.numpy as jnp
from jax import lax

NPB = 128
Q = 256
SEG_DEV = 256
NB_DEV = 384
NDEV = 32
CAP = 16
SEGMENTS = 8192
NB = 12288


def owner_routes(key):
    slot_count = NDEV * CAP
    hot_owner = jax.random.randint(jax.random.fold_in(key, 5), (), 0, NDEV)
    device_keys = jax.random.split(jax.random.fold_in(key, 7), NDEV)

    def one_device(dev_key):
        first, second, third = jax.random.split(dev_key, 3)
        positions = jnp.arange(slot_count, dtype=jnp.int32)
        scores = jax.random.randint(first, (slot_count,), 0, 65536) * slot_count + positions
        scores = jnp.where(positions // CAP == hot_owner, scores + 2 ** 30, scores)
        chosen = jax.lax.top_k(scores, SEG_DEV)[1]
        owners = (chosen // CAP).astype(jnp.int32)
        owners = jax.random.permutation(second, owners)
        local_ids = jax.random.randint(third, (SEG_DEV,), 0, NB_DEV)
        return owners * NB_DEV + local_ids
    return jax.vmap(one_device)(device_keys).reshape(-1).astype(jnp.int32)


def draw_sec_block(key, part):
    return owner_routes(jax.random.fold_in(key, 11))


def draw_pri_block(key, part):
    return owner_routes(jax.random.fold_in(key, 23))


def set_ends(array, key, least, high):
    longest = array.shape.index(max(array.shape))
    spots = []
    for shift in (0, 1):
        where = [jax.random.randint(jax.random.fold_in(key, axis), (), 0, length) for axis, length in enumerate(array.shape)]
        where[longest] = (where[longest] + shift) % array.shape[longest]
        spots.append(tuple(where))
    return array.at[spots[0]].set(least).at[spots[1]].set(high)


def levels(stream_key, dims, cuts, smallest, largest):
    gain = 1.0
    for dim, blocks in cuts:
        steps = jax.random.uniform(jax.random.fold_in(jax.random.fold_in(stream_key, 6), dim), (blocks,), jnp.float32, smallest / len(cuts), largest / len(cuts))
        gain = gain * jnp.repeat(jnp.exp(steps), dims[dim] // blocks).reshape((-1,) + (1,) * (len(dims) - 1 - dim))
    return gain


def normal_values(key, shape, width, limit, pieces=(), kind=jnp.bfloat16):
    values = jax.random.normal(key, shape, jnp.float32) * width
    if len(pieces) > 0:
        values = levels(key, shape, pieces, -0.22, 0.18) * values
    return jnp.clip(values, min=-limit, max=limit).astype(kind)


def setup_inputs(seed: int = 0) -> dict:
    keys = jax.random.split(jax.random.key(seed), 8)
    node_coords = normal_values(keys[0], (NB, 3, NPB), 1.0, 6.0, ((0, 32),), jnp.float32)
    node_disp = normal_values(keys[1], (NB, 3, NPB), 1.0, 6.0, ((0, 32),), jnp.float32)
    qpoints = normal_values(keys[2], (SEGMENTS, 3, Q), 1.0, 6.0, ((0, 32),), jnp.float32)
    qweights = jnp.clip(jnp.exp(math.log(2.0) - 2.9957323 * jax.random.uniform(keys[3], (SEGMENTS, Q), jnp.float32) ** levels(keys[3], (SEGMENTS, Q), ((0, 32),), -0.2, 0.2)), 0.1, 2.0)
    qcount = set_ends(jax.random.randint(keys[4], (SEGMENTS,), Q // 4, Q + 1), jax.random.fold_in(keys[4], 1), Q // 4, Q).astype(jnp.int32)
    sec_block = draw_sec_block(jax.random.fold_in(keys[7], 71), 0)
    pri_block = draw_pri_block(jax.random.fold_in(keys[7], 71), 0)
    return {"node_coords": node_coords, "node_disp": node_disp, "qpoints": qpoints, "qweights": qweights, "qcount": qcount, "sec_block": sec_block, "pri_block": pri_block}


def shape_values(points, coords):
    diff0 = points[:, 0, :, None] - coords[:, 0, None, :]
    diff1 = points[:, 1, :, None] - coords[:, 1, None, :]
    diff2 = points[:, 2, :, None] - coords[:, 2, None, :]
    radius = diff0 * diff0 + diff1 * diff1 + diff2 * diff2
    kernel = 1.0 / (1.0 + 2.0 * radius)
    return kernel / jnp.sum(kernel, axis=-1, keepdims=True)


def reference(node_coords, node_disp, qpoints, qweights, qcount, sec_block, pri_block):
    node_data = jnp.concatenate([node_coords, node_disp], axis=1)
    live = jnp.arange(Q, dtype=jnp.int32)[None, :] < qcount[:, None]
    weights = jnp.where(live, qweights, jnp.zeros_like(qweights))
    seg_group = 64
    groups = SEGMENTS // seg_group
    hp = lax.Precision.HIGHEST

    def one_group(inputs):
        points, quad_weights, sec_ids, pri_ids = inputs
        sec_nodes = jnp.take(node_data, sec_ids, axis=0)
        pri_nodes = jnp.take(node_data, pri_ids, axis=0)
        sec_shape = shape_values(points, sec_nodes[:, :3])
        pri_shape = shape_values(points, pri_nodes[:, :3])
        weighted = quad_weights[:, :, None] * sec_shape
        mismatch = jnp.einsum("gqj,gcj->gcq", sec_shape, sec_nodes[:, 3:], precision=hp) - jnp.einsum("gqj,gcj->gcq", pri_shape, pri_nodes[:, 3:], precision=hp)
        return jnp.einsum("gqk,gcq->gck", weighted, mismatch, precision=hp)

    contrib = lax.map(one_group, (qpoints.reshape(groups, seg_group, 3, Q), weights.reshape(groups, seg_group, Q), sec_block.reshape(groups, seg_group), pri_block.reshape(groups, seg_group)))
    contrib = contrib.reshape(SEGMENTS, 3, NPB)
    return jax.ops.segment_sum(contrib, sec_block, num_segments=NB)
```

```python
import functools
import jax
import jax.numpy as jnp
from jax import lax
from jax.experimental import pallas as pl
from jax.experimental.pallas import tpu as pltpu
from jax.sharding import PartitionSpec as P

GROUP = 8
UNROLL = 8


def routing(block_ids, blocks_dev, capacity, slot_count):
    owners = block_ids // blocks_dev
    local_ids = block_ids % blocks_dev
    positions = jnp.arange(block_ids.shape[0], dtype=jnp.int32)
    same_owner = (owners[:, None] == owners[None, :]) & (positions[:, None] > positions[None, :])
    ranks = jnp.sum(same_owner.astype(jnp.int32), axis=1)
    slot_ids = owners * capacity + ranks
    matches = slot_ids[:, None] == jnp.arange(slot_count, dtype=jnp.int32)[None, :]
    request = jnp.sum(jnp.where(matches, local_ids[:, None], 0), axis=0)
    return slot_ids, request


def exchange(x):
    return lax.all_to_all(x, ("gx", "gy"), split_axis=0, concat_axis=0, tiled=True)


def gather_kernel(sec_ids, pri_ids, table, out):
    width = table.shape[1]

    @pl.loop(0, out.shape[0])
    def _(i):
        for j in range(UNROLL):
            s = i * UNROLL + j
            out[i, j : j + 1, :width] = table[pl.ds(sec_ids[s], 1), :]
            out[i, j : j + 1, width:] = table[pl.ds(pri_ids[s], 1), :]


def gather_rows(sec_ids, pri_ids, table):
    rows, width = sec_ids.shape[0], table.shape[1]
    return pl.pallas_call(
        gather_kernel,
        out_shape=jax.ShapeDtypeStruct((rows // UNROLL, UNROLL, 2 * width), jnp.float32),
        in_specs=[
            pl.BlockSpec(memory_space=pltpu.SMEM),
            pl.BlockSpec(memory_space=pltpu.SMEM),
            pl.BlockSpec(memory_space=pltpu.VMEM),
        ],
        out_specs=pl.BlockSpec(memory_space=pltpu.VMEM),
        name="gather_rows",
    )(sec_ids, pri_ids, table).reshape(rows, 2 * width)


def rounded(x):
    return x.astype(jnp.bfloat16).astype(jnp.float32)


def stack_rows(rows, iota):
    out = jnp.zeros(iota.shape, jnp.float32)
    for i, row in rows:
        out = jnp.where(iota == i, row, out)
    return out


def coupling_kernel(sec_slots, pri_slots, nodes, feats, weights, parcels):
    n = nodes.shape[1] // 12
    step = pl.program_id(0)

    @pl.when(step == 0)
    def _():
        parcels[...] = jnp.zeros_like(parcels)

    iota2 = lax.broadcasted_iota(jnp.int32, (8, 2 * n), 0)
    iota1 = lax.broadcasted_iota(jnp.int32, (8, n), 0)
    iotaq = lax.broadcasted_iota(jnp.int32, (8, feats.shape[2]), 0)
    bf = jnp.bfloat16
    f32 = jnp.float32

    def disp_rows(row):
        u = [row[:, (3 + c) * n : (4 + c) * n] for c in range(3)]
        full = stack_rows([(i + 4 * h, u[i]) for h in range(2) for i in range(3)], iota1)
        full = jnp.where((iota1 == 3) | (iota1 == 7), 1.0, full)
        high = rounded(full)
        both = jnp.where(iota1 < 4, high, full - high).astype(bf)
        return jnp.concatenate([both, both], axis=1)

    for g in range(feats.shape[0]):
        seg = step * feats.shape[0] + g
        slot = sec_slots[seg]
        sec = nodes[pl.ds(slot, 1), : 6 * n]
        pri = nodes[pl.ds(pri_slots[seg], 1), 6 * n :]
        x = [
            jnp.concatenate([sec[:, c * n : (c + 1) * n], pri[:, c * n : (c + 1) * n]], axis=1)
            for c in range(3)
        ]
        square = 2.0 * (x[0] * x[0] + x[1] * x[1] + x[2] * x[2])
        full = stack_rows(
            [(0, -4.0 * x[0]), (1, -4.0 * x[1]), (2, -4.0 * x[2]), (3, square), (4, 1.0)], iota2
        )
        high = rounded(full)
        rest = full - high
        mid = rounded(rest)
        low = rest - mid
        left = jnp.concatenate([high, high, mid, high, low, mid], axis=0)
        left = left.T.astype(bf)
        denom = jnp.dot(left, feats[g], preferred_element_type=f32)
        kern = 1.0 / denom
        kh = kern.astype(bf)
        kl = (kern - kh.astype(f32)).astype(bf)
        p1 = jnp.concatenate([kh[:n], kl[:n]], axis=0)
        p2 = jnp.concatenate([kh[n:], kl[n:]], axis=0)
        a1 = jnp.dot(disp_rows(sec), p1, preferred_element_type=f32)
        a2 = jnp.dot(disp_rows(pri), p2, preferred_element_type=f32)
        t1 = a1 + pltpu.roll(a1, 4, 0)
        t2 = a2 + pltpu.roll(a2, 4, 0)
        r1 = 1.0 / t1[3:4]
        r2 = 1.0 / t2[3:4]
        gap = (t1 * r1 - t2 * r2) * (weights[g : g + 1] * r1)
        high = rounded(gap)
        gap = jnp.where(iotaq < 4, high, gap - high).astype(bf)
        c = lax.dot_general(gap, p1, (((1,), (1,)), ((), ())), preferred_element_type=f32)
        c = c[:, :n] + c[:, n:]
        c = c + pltpu.roll(c, 4, 0)
        parcels[slot] = c[:3]


def coupling(sec_slots, pri_slots, nodes, feats, weights):
    segs, depth, points = feats.shape
    slots, width = nodes.shape
    node_count = width // 12
    return pl.pallas_call(
        coupling_kernel,
        grid_spec=pltpu.PrefetchScalarGridSpec(
            num_scalar_prefetch=2,
            grid=(segs // GROUP,),
            in_specs=[
                pl.BlockSpec((slots, width), lambda i, *_: (0, 0)),
                pl.BlockSpec((GROUP, depth, points), lambda i, *_: (i, 0, 0)),
                pl.BlockSpec((GROUP, points), lambda i, *_: (i, 0)),
            ],
            out_specs=pl.BlockSpec((slots, 3, node_count), lambda i, *_: (0, 0, 0)),
        ),
        out_shape=jax.ShapeDtypeStruct((slots, 3, node_count), jnp.float32),
        name="coupling",
    )(sec_slots, pri_slots, nodes, feats, weights).reshape(slots, 3 * node_count)


def assemble_kernel(ids, incoming, gap):
    blocks, comps, n = gap.shape
    slots = incoming.shape[0]
    match = lax.broadcasted_iota(jnp.int32, (blocks, slots), 0) == ids[...]
    select = jnp.where(match, 1.0, 0.0).astype(jnp.bfloat16)
    for c in range(comps):
        x = incoming[:, c * n : (c + 1) * n]
        high = rounded(x)
        rest = x - high
        mid = rounded(rest)
        pieces = jnp.concatenate([high, mid, rest - mid], axis=1).astype(jnp.bfloat16)
        y = jnp.dot(select, pieces, preferred_element_type=jnp.float32)
        gap[:, c, :] = y[:, :n] + (y[:, n : 2 * n] + y[:, 2 * n :])


def assemble(ids, incoming, blocks, comps):
    n = incoming.shape[1] // comps
    return pl.pallas_call(
        assemble_kernel,
        out_shape=jax.ShapeDtypeStruct((blocks, comps, n), jnp.float32),
        in_specs=[pl.BlockSpec(memory_space=pltpu.VMEM)] * 2,
        out_specs=pl.BlockSpec(memory_space=pltpu.VMEM),
        name="assemble",
    )(ids[None, :], incoming)


def point_features(qpoints):
    square = 1.0 + 2.0 * jnp.sum(qpoints * qpoints, axis=1, keepdims=True)
    ones = jnp.ones_like(square)
    full = jnp.concatenate([qpoints, ones, square, jnp.zeros_like(qpoints)], axis=1)
    high = lax.reduce_precision(full, 8, 7)
    rest = full - high
    mid = lax.reduce_precision(rest, 8, 7)
    low = rest - mid
    return jnp.concatenate([high, mid, high, low, high, mid], axis=1).astype(jnp.bfloat16)


def body(node_coords, node_disp, qpoints, qweights, qcount, sec_block, pri_block):
    devices = lax.axis_size("gx") * lax.axis_size("gy")
    blocks_dev, comps, node_count = node_coords.shape
    seg_count = qpoints.shape[0]
    quad_points = qpoints.shape[2]
    slot_count = 2 * seg_count
    capacity = slot_count // devices
    sec_slots, sec_request = routing(sec_block, blocks_dev, capacity, slot_count)
    pri_slots, pri_request = routing(pri_block, blocks_dev, capacity, slot_count)
    requests = jnp.stack(
        [sec_request.reshape(devices, capacity), pri_request.reshape(devices, capacity)], axis=1
    )
    received = exchange(requests)
    sec_ids = received[:, 0].reshape(slot_count)
    pri_ids = received[:, 1].reshape(slot_count)
    table = jnp.concatenate(
        [node_coords.reshape(blocks_dev, -1), node_disp.reshape(blocks_dev, -1)], axis=1
    )
    nodes = exchange(gather_rows(sec_ids, pri_ids, table))
    live = jnp.arange(quad_points, dtype=jnp.int32)[None, :] < qcount[:, None]
    weights = jnp.where(live, qweights, jnp.zeros_like(qweights))
    parcels = coupling(sec_slots, pri_slots, nodes, point_features(qpoints), weights)
    return assemble(sec_ids, exchange(parcels), blocks_dev, comps)


def solution(mesh):
    placed = (
        P(("gx", "gy"), None, None),
        P(("gx", "gy"), None, None),
        P(("gx", "gy"), None, None),
        P(("gx", "gy"), None),
        P(("gx", "gy")),
        P(("gx", "gy")),
        P(("gx", "gy")),
    )
    return jax.shard_map(
        body, mesh=mesh, in_specs=placed, out_specs=P(("gx", "gy"), None, None), check_vma=False
    )
```

```python
import functools
import jax
import jax.numpy as jnp
from jax import lax
from jax.experimental import pallas as pl
from jax.experimental.pallas import tpu as pltpu
from jax.sharding import PartitionSpec as P

GROUP = 16
UNROLL = 8


def routing(block_ids, blocks_dev, capacity, slot_count):
    owners = block_ids // blocks_dev
    local_ids = block_ids % blocks_dev
    positions = jnp.arange(block_ids.shape[0], dtype=jnp.int32)
    same_owner = (owners[:, None] == owners[None, :]) & (positions[:, None] > positions[None, :])
    ranks = jnp.sum(same_owner.astype(jnp.int32), axis=1)
    slot_ids = owners * capacity + ranks
    matches = slot_ids[:, None] == jnp.arange(slot_count, dtype=jnp.int32)[None, :]
    request = jnp.sum(jnp.where(matches, local_ids[:, None], 0), axis=0)
    return slot_ids, request


def exchange(x):
    return lax.all_to_all(x, ("gx", "gy"), split_axis=0, concat_axis=0, tiled=True)


def gather_kernel(ids, coords, disp, out):
    comps, _, n = coords.shape

    @pl.loop(0, out.shape[0])
    def _(i):
        for j in range(UNROLL):
            b = ids[i * UNROLL + j]
            for c in range(comps):
                out[i, j : j + 1, c * n : (c + 1) * n] = coords[c, pl.ds(b, 1), :]
                k = comps + c
                out[i, j : j + 1, k * n : (k + 1) * n] = disp[c, pl.ds(b, 1), :]


def gather_rows(ids, coords, disp):
    rows, width = ids.shape[0], 2 * coords.shape[0] * coords.shape[2]
    return pl.pallas_call(
        gather_kernel,
        out_shape=jax.ShapeDtypeStruct((rows // UNROLL, UNROLL, width), jnp.float32),
        in_specs=[
            pl.BlockSpec(memory_space=pltpu.SMEM),
            pl.BlockSpec(memory_space=pltpu.VMEM),
            pl.BlockSpec(memory_space=pltpu.VMEM),
        ],
        out_specs=pl.BlockSpec(memory_space=pltpu.VMEM),
        name="gather_rows",
    )(ids, coords, disp).reshape(rows, width)


def rounded(x):
    return x.astype(jnp.bfloat16).astype(jnp.float32)


def stack_rows(rows, iota):
    out = jnp.zeros(iota.shape, jnp.float32)
    for i, row in rows:
        out = jnp.where(iota == i, row, out)
    return out


def disp_rows(row, n):
    iota = lax.broadcasted_iota(jnp.int32, (8, n), 0)
    u = [row[:, (3 + c) * n : (4 + c) * n] for c in range(3)]
    full = stack_rows([(i + 4 * h, u[i]) for h in range(2) for i in range(3)], iota)
    full = jnp.where((iota == 3) | (iota == 7), 1.0, full)
    both = jnp.where(iota < 4, rounded(full), full - rounded(full)).astype(jnp.bfloat16)
    return jnp.concatenate([both, both], axis=1)


def side(row, feat, n):
    bf, f32 = jnp.bfloat16, jnp.float32
    iota = lax.broadcasted_iota(jnp.int32, (8, n), 0)
    x = [row[:, c * n : (c + 1) * n] for c in range(3)]
    square = 2.0 * (x[0] * x[0] + x[1] * x[1] + x[2] * x[2])
    full = stack_rows(
        [(0, -4.0 * x[0]), (1, -4.0 * x[1]), (2, -4.0 * x[2]), (3, square), (4, 1.0)], iota
    )
    high = rounded(full)
    rest = full - high
    mid = rounded(rest)
    left = jnp.concatenate([high, high, mid, high, rest - mid, mid], axis=0)
    kern = 1.0 / jnp.dot(left.T.astype(bf), feat, preferred_element_type=f32)
    kh = kern.astype(bf)
    kl = (kern - kh.astype(f32)).astype(bf)
    both = jnp.concatenate([kh, kl], axis=0)
    a = jnp.dot(disp_rows(row, n), both, preferred_element_type=f32)
    total = a + pltpu.roll(a, 4, 0)
    inv = 1.0 / total[3:4]
    return both, total * inv, inv


def pri_kernel(slots, nodes, feats, means):
    n = nodes.shape[1] // 6
    for g in range(feats.shape[0]):
        row = nodes[pl.ds(slots[pl.program_id(0) * feats.shape[0] + g], 1), :]
        means[g] = side(row, feats[g], n)[1]


def sec_kernel(slots, nodes, feats, weights, means, parcels):
    n = nodes.shape[1] // 6
    step = pl.program_id(0)

    @pl.when(step == 0)
    def _():
        parcels[...] = jnp.zeros_like(parcels)

    iota = lax.broadcasted_iota(jnp.int32, (8, feats.shape[2]), 0)
    for g in range(feats.shape[0]):
        slot = slots[step * feats.shape[0] + g]
        both, mean, inv = side(nodes[pl.ds(slot, 1), :], feats[g], n)
        gap = (mean - means[g]) * (weights[g : g + 1] * inv)
        high = rounded(gap)
        gap = jnp.where(iota < 4, high, gap - high).astype(jnp.bfloat16)
        c = lax.dot_general(
            gap, both, (((1,), (1,)), ((), ())), preferred_element_type=jnp.float32
        )
        c = c[:, :n] + c[:, n:]
        c = c + pltpu.roll(c, 4, 0)
        parcels[slot] = c[:3]


def cost(segs, points, n):
    return pl.CostEstimate(
        flops=8 * segs * points * n * 16, bytes_accessed=segs * points * 128, transcendentals=0
    )


def pri_means(slots_of, nodes, feats):
    segs, depth, points = feats.shape
    slots, width = nodes.shape
    return pl.pallas_call(
        pri_kernel,
        grid_spec=pltpu.PrefetchScalarGridSpec(
            num_scalar_prefetch=1,
            grid=(segs // GROUP,),
            in_specs=[
                pl.BlockSpec((slots, width), lambda i, *_: (0, 0)),
                pl.BlockSpec((GROUP, depth, points), lambda i, *_: (i, 0, 0)),
            ],
            out_specs=pl.BlockSpec((GROUP, 8, points), lambda i, *_: (i, 0, 0)),
        ),
        out_shape=jax.ShapeDtypeStruct((segs, 8, points), jnp.float32),
        cost_estimate=cost(segs, points, width // 6),
        name="pri_means",
    )(slots_of, nodes, feats)


def coupling(slots_of, nodes, feats, weights, means):
    segs, depth, points = feats.shape
    slots, width = nodes.shape
    n = width // 6
    return pl.pallas_call(
        sec_kernel,
        grid_spec=pltpu.PrefetchScalarGridSpec(
            num_scalar_prefetch=1,
            grid=(segs // GROUP,),
            in_specs=[
                pl.BlockSpec((slots, width), lambda i, *_: (0, 0)),
                pl.BlockSpec((GROUP, depth, points), lambda i, *_: (i, 0, 0)),
                pl.BlockSpec((GROUP, points), lambda i, *_: (i, 0)),
                pl.BlockSpec((GROUP, 8, points), lambda i, *_: (i, 0, 0)),
            ],
            out_specs=pl.BlockSpec((slots, 3, n), lambda i, *_: (0, 0, 0)),
        ),
        out_shape=jax.ShapeDtypeStruct((slots, 3, n), jnp.float32),
        cost_estimate=cost(segs, points, n),
        name="coupling",
    )(slots_of, nodes, feats, weights, means).reshape(slots, 3 * n)


def assemble_kernel(ids, incoming, gap):
    comps, blocks, n = gap.shape
    slots = incoming.shape[0]
    match = lax.broadcasted_iota(jnp.int32, (blocks, slots), 0) == ids[...]
    select = jnp.where(match, 1.0, 0.0).astype(jnp.bfloat16)
    for c in range(comps):
        x = incoming[:, c * n : (c + 1) * n]
        high = rounded(x)
        rest = x - high
        mid = rounded(rest)
        pieces = jnp.concatenate([high, mid, rest - mid], axis=1).astype(jnp.bfloat16)
        y = jnp.dot(select, pieces, preferred_element_type=jnp.float32)
        gap[c] = y[:, :n] + (y[:, n : 2 * n] + y[:, 2 * n :])


def assemble(ids, incoming, blocks, comps):
    n = incoming.shape[1] // comps
    return pl.pallas_call(
        assemble_kernel,
        out_shape=jax.ShapeDtypeStruct((comps, blocks, n), jnp.float32),
        in_specs=[pl.BlockSpec(memory_space=pltpu.VMEM)] * 2,
        out_specs=pl.BlockSpec(memory_space=pltpu.VMEM),
        name="assemble",
    )(ids[None, :], incoming).transpose(1, 0, 2)


def point_features(qpoints):
    square = 1.0 + 2.0 * jnp.sum(qpoints * qpoints, axis=1, keepdims=True)
    ones = jnp.ones_like(square)
    full = jnp.concatenate([qpoints, ones, square, jnp.zeros_like(qpoints)], axis=1)
    high = lax.reduce_precision(full, 8, 7)
    rest = full - high
    mid = lax.reduce_precision(rest, 8, 7)
    low = rest - mid
    return jnp.concatenate([high, mid, high, low, high, mid], axis=1).astype(jnp.bfloat16)


def body(node_coords, node_disp, qpoints, qweights, qcount, sec_block, pri_block):
    devices = lax.axis_size("gx") * lax.axis_size("gy")
    blocks_dev, comps, node_count = node_coords.shape
    seg_count = qpoints.shape[0]
    quad_points = qpoints.shape[2]
    slot_count = 2 * seg_count
    capacity = slot_count // devices
    sec_slots, sec_request = routing(sec_block, blocks_dev, capacity, slot_count)
    pri_slots, pri_request = routing(pri_block, blocks_dev, capacity, slot_count)
    requests = jnp.stack(
        [sec_request.reshape(devices, capacity), pri_request.reshape(devices, capacity)], axis=1
    )
    received = exchange(requests)
    sec_ids = received[:, 0].reshape(slot_count)
    pri_ids = received[:, 1].reshape(slot_count)
    coords = node_coords.transpose(1, 0, 2)
    disp = node_disp.transpose(1, 0, 2)
    pri_nodes = exchange(gather_rows(pri_ids, coords, disp))
    sec_rows, feats, pri_nodes = lax.optimization_barrier(
        (gather_rows(sec_ids, coords, disp), point_features(qpoints), pri_nodes)
    )
    sec_nodes = exchange(sec_rows)
    live = jnp.arange(quad_points, dtype=jnp.int32)[None, :] < qcount[:, None]
    weights = jnp.where(live, qweights, jnp.zeros_like(qweights))
    means = pri_means(pri_slots, pri_nodes, feats)
    parcels = coupling(sec_slots, sec_nodes, feats, weights, means)
    return assemble(sec_ids, exchange(parcels), blocks_dev, comps)


def solution(mesh):
    placed = (
        P(("gx", "gy"), None, None),
        P(("gx", "gy"), None, None),
        P(("gx", "gy"), None, None),
        P(("gx", "gy"), None),
        P(("gx", "gy")),
        P(("gx", "gy")),
        P(("gx", "gy")),
    )
    return jax.shard_map(
        body, mesh=mesh, in_specs=placed, out_specs=P(("gx", "gy"), None, None), check_vma=False
    )
```

```python
import functools
import jax
import jax.numpy as jnp
from jax import lax
from jax.experimental import pallas as pl
from jax.experimental.pallas import tpu as pltpu
from jax.sharding import PartitionSpec as P

GROUP = 16
UNROLL = 8


def routing(block_ids, blocks_dev, capacity, slot_count):
    owners = block_ids // blocks_dev
    local_ids = block_ids % blocks_dev
    positions = jnp.arange(block_ids.shape[0], dtype=jnp.int32)
    same_owner = (owners[:, None] == owners[None, :]) & (positions[:, None] > positions[None, :])
    ranks = jnp.sum(same_owner.astype(jnp.int32), axis=1)
    slot_ids = owners * capacity + ranks
    matches = slot_ids[:, None] == jnp.arange(slot_count, dtype=jnp.int32)[None, :]
    request = jnp.sum(jnp.where(matches, local_ids[:, None], 0), axis=0)
    return slot_ids, request


def exchange(x):
    return lax.all_to_all(x, ("gx", "gy"), split_axis=0, concat_axis=0, tiled=True)


def gather_kernel(ids, coords, disp, out):
    comps, _, n = coords.shape

    @pl.loop(0, out.shape[0])
    def _(i):
        for j in range(UNROLL):
            b = ids[i * UNROLL + j]
            for c in range(comps):
                out[i, j : j + 1, c * n : (c + 1) * n] = coords[c, pl.ds(b, 1), :]
                k = comps + c
                out[i, j : j + 1, k * n : (k + 1) * n] = disp[c, pl.ds(b, 1), :]


def gather_rows(ids, coords, disp):
    rows, width = ids.shape[0], 2 * coords.shape[0] * coords.shape[2]
    return pl.pallas_call(
        gather_kernel,
        out_shape=jax.ShapeDtypeStruct((rows // UNROLL, UNROLL, width), jnp.float32),
        in_specs=[
            pl.BlockSpec(memory_space=pltpu.SMEM),
            pl.BlockSpec(memory_space=pltpu.VMEM),
            pl.BlockSpec(memory_space=pltpu.VMEM),
        ],
        out_specs=pl.BlockSpec(memory_space=pltpu.VMEM),
        name="gather_rows",
    )(ids, coords, disp).reshape(rows, width)


def rounded(x):
    return x.astype(jnp.bfloat16).astype(jnp.float32)


def stack_rows(rows, iota):
    out = jnp.zeros(iota.shape, jnp.float32)
    for i, row in rows:
        out = jnp.where(iota == i, row, out)
    return out


def disp_rows(row, n):
    iota = lax.broadcasted_iota(jnp.int32, (8, n), 0)
    u = [row[:, (3 + c) * n : (4 + c) * n] for c in range(3)]
    full = stack_rows([(i + 4 * h, u[i]) for h in range(2) for i in range(3)], iota)
    full = jnp.where((iota == 3) | (iota == 7), 1.0, full)
    both = jnp.where(iota < 4, rounded(full), full - rounded(full)).astype(jnp.bfloat16)
    return jnp.concatenate([both, both], axis=1)


def side(row, feat, n):
    bf, f32 = jnp.bfloat16, jnp.float32
    iota = lax.broadcasted_iota(jnp.int32, (8, n), 0)
    x = [row[:, c * n : (c + 1) * n] for c in range(3)]
    square = 2.0 * (x[0] * x[0] + x[1] * x[1] + x[2] * x[2])
    full = stack_rows(
        [(0, -4.0 * x[0]), (1, -4.0 * x[1]), (2, -4.0 * x[2]), (3, square), (4, 1.0)], iota
    )
    high = rounded(full)
    rest = full - high
    mid = rounded(rest)
    left = jnp.concatenate([high, high, mid, high, rest - mid, mid], axis=0)
    kern = 1.0 / jnp.dot(left.T.astype(bf), feat, preferred_element_type=f32)
    kh = kern.astype(bf)
    kl = (kern - kh.astype(f32)).astype(bf)
    both = jnp.concatenate([kh, kl], axis=0)
    a = jnp.dot(disp_rows(row, n), both, preferred_element_type=f32)
    total = a + pltpu.roll(a, 4, 0)
    inv = 1.0 / total[3:4]
    return both, total * inv, inv


def pri_kernel(slots, nodes, feats, means):
    n = nodes.shape[1] // 6
    for g in range(feats.shape[0]):
        row = nodes[pl.ds(slots[pl.program_id(0) * feats.shape[0] + g], 1), :]
        means[g] = side(row, feats[g], n)[1]


def sec_kernel(slots, nodes, feats, weights, means, parcels):
    n = nodes.shape[1] // 6
    step = pl.program_id(0)

    @pl.when(step == 0)
    def _():
        parcels[...] = jnp.zeros_like(parcels)

    iota = lax.broadcasted_iota(jnp.int32, (8, feats.shape[2]), 0)
    for g in range(feats.shape[0]):
        slot = slots[step * feats.shape[0] + g]
        both, mean, inv = side(nodes[pl.ds(slot, 1), :], feats[g], n)
        gap = (mean - means[g]) * (weights[g : g + 1] * inv)
        high = rounded(gap)
        gap = jnp.where(iota < 4, high, gap - high).astype(jnp.bfloat16)
        c = lax.dot_general(
            both, gap, (((1,), (1,)), ((), ())), preferred_element_type=jnp.float32
        )
        c = (c[:n] + c[n:]).T
        c = c + pltpu.roll(c, 4, 0)
        parcels[slot] = c[:3]


def cost(segs, points, n):
    return pl.CostEstimate(
        flops=8 * segs * points * n * 16, bytes_accessed=segs * points * 128, transcendentals=0
    )


def pri_means(slots_of, nodes, feats):
    segs, depth, points = feats.shape
    slots, width = nodes.shape
    return pl.pallas_call(
        pri_kernel,
        grid_spec=pltpu.PrefetchScalarGridSpec(
            num_scalar_prefetch=1,
            grid=(segs // GROUP,),
            in_specs=[
                pl.BlockSpec((slots, width), lambda i, *_: (0, 0)),
                pl.BlockSpec((GROUP, depth, points), lambda i, *_: (i, 0, 0)),
            ],
            out_specs=pl.BlockSpec((GROUP, 8, points), lambda i, *_: (i, 0, 0)),
        ),
        out_shape=jax.ShapeDtypeStruct((segs, 8, points), jnp.float32),
        cost_estimate=cost(segs, points, width // 6),
        name="pri_means",
    )(slots_of, nodes, feats)


def coupling(slots_of, nodes, feats, weights, means):
    segs, depth, points = feats.shape
    slots, width = nodes.shape
    n = width // 6
    return pl.pallas_call(
        sec_kernel,
        grid_spec=pltpu.PrefetchScalarGridSpec(
            num_scalar_prefetch=1,
            grid=(segs // GROUP,),
            in_specs=[
                pl.BlockSpec((slots, width), lambda i, *_: (0, 0)),
                pl.BlockSpec((GROUP, depth, points), lambda i, *_: (i, 0, 0)),
                pl.BlockSpec((GROUP, points), lambda i, *_: (i, 0)),
                pl.BlockSpec((GROUP, 8, points), lambda i, *_: (i, 0, 0)),
            ],
            out_specs=pl.BlockSpec((slots, 3, n), lambda i, *_: (0, 0, 0)),
        ),
        out_shape=jax.ShapeDtypeStruct((slots, 3, n), jnp.float32),
        cost_estimate=cost(segs, points, n),
        name="coupling",
    )(slots_of, nodes, feats, weights, means).reshape(slots, 3 * n)


def assemble_kernel(ids, incoming, gap):
    comps, blocks, n = gap.shape
    slots = incoming.shape[0]
    match = lax.broadcasted_iota(jnp.int32, (blocks, slots), 0) == ids[...]
    select = jnp.where(match, 1.0, 0.0).astype(jnp.bfloat16)
    for c in range(comps):
        x = incoming[:, c * n : (c + 1) * n]
        high = rounded(x)
        rest = x - high
        mid = rounded(rest)
        pieces = jnp.concatenate([high, mid, rest - mid], axis=1).astype(jnp.bfloat16)
        y = jnp.dot(select, pieces, preferred_element_type=jnp.float32)
        gap[c] = y[:, :n] + (y[:, n : 2 * n] + y[:, 2 * n :])


def assemble(ids, incoming, blocks, comps):
    n = incoming.shape[1] // comps
    return pl.pallas_call(
        assemble_kernel,
        out_shape=jax.ShapeDtypeStruct((comps, blocks, n), jnp.float32),
        in_specs=[pl.BlockSpec(memory_space=pltpu.VMEM)] * 2,
        out_specs=pl.BlockSpec(memory_space=pltpu.VMEM),
        name="assemble",
    )(ids[None, :], incoming).transpose(1, 0, 2)


def point_features(qpoints):
    square = 1.0 + 2.0 * jnp.sum(qpoints * qpoints, axis=1, keepdims=True)
    ones = jnp.ones_like(square)
    full = jnp.concatenate([qpoints, ones, square, jnp.zeros_like(qpoints)], axis=1)
    high = lax.reduce_precision(full, 8, 7)
    rest = full - high
    mid = lax.reduce_precision(rest, 8, 7)
    low = rest - mid
    return jnp.concatenate([high, mid, high, low, high, mid], axis=1).astype(jnp.bfloat16)


def body(node_coords, node_disp, qpoints, qweights, qcount, sec_block, pri_block):
    devices = lax.axis_size("gx") * lax.axis_size("gy")
    blocks_dev, comps, node_count = node_coords.shape
    seg_count = qpoints.shape[0]
    quad_points = qpoints.shape[2]
    slot_count = 2 * seg_count
    capacity = slot_count // devices
    sec_slots, sec_request = routing(sec_block, blocks_dev, capacity, slot_count)
    pri_slots, pri_request = routing(pri_block, blocks_dev, capacity, slot_count)
    requests = jnp.stack(
        [sec_request.reshape(devices, capacity), pri_request.reshape(devices, capacity)], axis=1
    )
    received = exchange(requests)
    sec_ids = received[:, 0].reshape(slot_count)
    pri_ids = received[:, 1].reshape(slot_count)
    coords = node_coords.transpose(1, 0, 2)
    disp = node_disp.transpose(1, 0, 2)
    pri_nodes = exchange(gather_rows(pri_ids, coords, disp))
    sec_rows, feats, pri_nodes = lax.optimization_barrier(
        (gather_rows(sec_ids, coords, disp), point_features(qpoints), pri_nodes)
    )
    sec_nodes = exchange(sec_rows)
    live = jnp.arange(quad_points, dtype=jnp.int32)[None, :] < qcount[:, None]
    weights = jnp.where(live, qweights, jnp.zeros_like(qweights))
    means = pri_means(pri_slots, pri_nodes, feats)
    parcels = coupling(sec_slots, sec_nodes, feats, weights, means)
    return assemble(sec_ids, exchange(parcels), blocks_dev, comps)


def solution(mesh):
    placed = (
        P(("gx", "gy"), None, None),
        P(("gx", "gy"), None, None),
        P(("gx", "gy"), None, None),
        P(("gx", "gy"), None),
        P(("gx", "gy")),
        P(("gx", "gy")),
        P(("gx", "gy")),
    )
    return jax.shard_map(
        body, mesh=mesh, in_specs=placed, out_specs=P(("gx", "gy"), None, None), check_vma=False
    )
```
